32 devices in a mesh: dp: 4 (over z), expert: 8 (over y, x, core).
Axes of the slice: x: 2, y: 2, z: 4, core: 2. Of those that a mesh axis runs over, the one named last changes fastest.
Arguments:
- tokens: bfloat16 [2048, 2048], P(('dp', 'expert')), may hold values from -6 to 6
- norm_gain: bfloat16 [2048], replicated, may hold values from 0.099609375 to 1.8984375
- router_weight: bfloat16 [2048, 8], replicated, may hold values from -0.125 to 0.125
- gate_weight: bfloat16 [8, 2048, 5120], P('expert', None, 'dp'), may hold values from -0.125 to 0.125
- up_weight: bfloat16 [8, 2048, 5120], P('expert', None, 'dp'), may hold values from -0.125 to 0.125
- down_weight: bfloat16 [8, 5120, 2048], P('expert', 'dp'), may hold values from -0.078125 to 0.078125
- expert_picks: int32 [4, 8, 128], P('dp'), may hold values from 0 to 511, as said below
- final_gain: bfloat16 [2048], replicated, may hold values from 0.099609375 to 1.8984375
- kv_weight: bfloat16 [2048, 8, 6, 2, 64], P(None, 'expert'), may hold values from -0.125 to 0.125
Outputs:
- moe_out: bfloat16 [2048, 2048], P(('dp', 'expert'))
- kv_cache: bfloat16 [2048, 8, 6, 2, 64], P('dp', 'expert')
The draws below stay inside these ranges and needn't reach their ends.
Inputs may be any that keep to these rules, and one draw needn't show every extreme that they name: `expert_picks`: for each group and expert, 128 different positions in the group. Of the 64 tokens of one device (positions s * 64 to (s + 1) * 64 - 1) one expert picks at most 32, and for every group and expert some device's tokens are picked exactly 32 times.
All inputs are finite; a program needn't handle non-finite values.
Results may differ from the reference program's by a relative error of at most 0.013.
Values may be sent and summed in bfloat16 or wider, within the bound.
A program may use at most 128 MiB of HBM per device.

```python
import jax
import jax.numpy as jnp
from jax import lax

D = 2048
FF = 5120
DK = 64
TOK_DEV = 64
LAYERS = 6
EXPERTS = 8
HEADS = 8
TOKENS = 2048
CAP = 128
MOST = 32
N_DP = 4
N_EXPERT = 8


def one_expert_picks(sub_key):
    key_full, key_slot, key_perm, key_order = jax.random.split(sub_key, 4)
    full_shard = jax.random.randint(key_full, (), 0, N_EXPERT)
    scores = jax.random.permutation(key_slot, N_EXPERT * MOST).astype(jnp.int32)
    shard_of = jnp.arange(N_EXPERT * MOST, dtype=jnp.int32) // MOST
    scores = jnp.where(shard_of == full_shard, scores - N_EXPERT * MOST, scores)
    chosen = jnp.argsort(scores, stable=True)[:CAP].astype(jnp.int32)
    shard_pos = chosen // MOST
    within = chosen % MOST
    shard_perms = jax.vmap(lambda perm_key: jax.random.permutation(perm_key, TOK_DEV))(jax.random.split(key_perm, N_EXPERT))
    token_pos = shard_pos * TOK_DEV + shard_perms[shard_pos, within].astype(jnp.int32)
    pick_order = jax.random.permutation(key_order, CAP)
    return token_pos[pick_order].astype(jnp.int32)


def draw_expert_picks(key, part):
    base = jax.random.fold_in(key, 7)
    keys = jax.random.split(base, N_DP * EXPERTS)
    all_picks = jax.vmap(one_expert_picks)(keys)
    return all_picks.reshape(N_DP, EXPERTS, CAP).astype(jnp.int32)


def levels(own_key, shape, shards, smallest, high):
    def one(axis_at, parts):
        draws = jax.random.uniform(jax.random.fold_in(jax.random.fold_in(own_key, 6), axis_at), (parts,), jnp.float32, smallest / len(shards), high / len(shards))
        return jnp.repeat(jnp.exp(draws), shape[axis_at] // parts).reshape((-1,) + (1,) * (len(shape) - axis_at - 1))

    level = one(*shards[0])
    for cut in shards[1:]:
        level = level * one(*cut)
    return level


def gaussian(key, dims, scale, bound, cuts=(), kind=jnp.bfloat16):
    level = levels(key, dims, cuts, -0.22, 0.18) if cuts else 1.0
    entries = jax.random.normal(key, dims, jnp.float32) * scale * level
    return jnp.minimum(jnp.maximum(entries, -bound), bound).astype(kind)


def setup_inputs(seed: int = 0) -> dict:
    key_list = jax.random.split(jax.random.key(seed), 10)
    tokens = gaussian(key_list[0], (TOKENS, D), 1.0, 6.0, ((0, 32),))
    norm_gain = jnp.clip(1.0 + 0.18 * jax.random.normal(key_list[1], (D,), jnp.float32), 0.099609375, 1.8984375).astype(jnp.bfloat16)
    router_weight = gaussian(key_list[2], (D, EXPERTS), D ** -0.5, 0.125)
    gate_weight = gaussian(key_list[3], (EXPERTS, D, FF), D ** -0.5, 0.125, ((0, 8), (2, 4)))
    up_weight = gaussian(key_list[4], (EXPERTS, D, FF), D ** -0.5, 0.125, ((0, 8), (2, 4)))
    down_weight = gaussian(key_list[5], (EXPERTS, FF, D), FF ** -0.5, 0.078125, ((0, 8), (1, 4)))
    expert_picks = draw_expert_picks(jax.random.fold_in(key_list[9], 71), 0)
    final_gain = jnp.clip(1.0 + 0.18 * jax.random.normal(key_list[7], (D,), jnp.float32), 0.099609375, 1.8984375).astype(jnp.bfloat16)
    kv_weight = gaussian(key_list[8], (D, HEADS, LAYERS, 2, DK), D ** -0.5, 0.125, ((1, 8),))
    return {"tokens": tokens, "norm_gain": norm_gain, "router_weight": router_weight, "gate_weight": gate_weight, "up_weight": up_weight, "down_weight": down_weight, "expert_picks": expert_picks, "final_gain": final_gain, "kv_weight": kv_weight}


def normalize(values, gain):
    return values * lax.rsqrt(lax.optimization_barrier(jnp.mean(values * values, axis=-1, keepdims=True)) + 1e-06) * gain.astype(jnp.float32)

def reference(tokens, norm_gain, router_weight, gate_weight, up_weight, down_weight, expert_picks, final_gain, kv_weight):
    wide_tokens = tokens.astype(jnp.float32)
    normed = normalize(wide_tokens, norm_gain).astype(jnp.bfloat16)
    gate_probs = jax.nn.sigmoid(jnp.dot(normed, router_weight, preferred_element_type=jnp.float32))
    group_start = jnp.arange(N_DP, dtype=jnp.int32)[:, None, None] * (TOK_DEV * N_EXPERT)
    all_rows = jnp.transpose(group_start + expert_picks, (1, 0, 2)).reshape(EXPERTS, -1).astype(jnp.int32)
    block_width = FF // N_DP

    def one_expert(expert):
        row_index = lax.dynamic_index_in_dim(all_rows, expert, 0, keepdims=False)
        inputs = normed[row_index]
        gate_act = jnp.dot(inputs, gate_weight[expert], preferred_element_type=jnp.float32)
        up_act = jnp.dot(inputs, up_weight[expert], preferred_element_type=jnp.float32)
        hidden = (jax.nn.gelu(gate_act, approximate=True) * up_act).astype(jnp.bfloat16)
        down_here = down_weight[expert]
        total = jnp.zeros((hidden.shape[0], D), jnp.float32)
        for block in range(N_DP):
            partial_sum = jnp.dot(hidden[:, block * block_width:(block + 1) * block_width], down_here[block * block_width:(block + 1) * block_width], preferred_element_type=jnp.float32).astype(jnp.bfloat16)
            partial_sum = lax.optimization_barrier(partial_sum)
            total = total + partial_sum.astype(jnp.float32)
        result = total.astype(jnp.bfloat16)
        weight = gate_probs[row_index, expert]
        return result.astype(jnp.float32) * weight[:, None]
    contributions = lax.map(one_expert, jnp.arange(EXPERTS, dtype=jnp.int32))
    combined = jnp.zeros((TOKENS, D), jnp.float32).at[all_rows.reshape(-1)].add(contributions.reshape(-1, D))
    moe_out = (wide_tokens + combined).astype(jnp.bfloat16)
    encoded = normalize(moe_out.astype(jnp.float32), final_gain).astype(jnp.bfloat16)
    projected = jnp.dot(encoded, kv_weight.reshape(D, -1), preferred_element_type=jnp.float32).astype(jnp.bfloat16)
    kv_cache = projected.reshape(TOKENS, HEADS, LAYERS, 2, DK)
    return (moe_out, kv_cache)
```

```python
import functools

import jax
import jax.numpy as jnp
from jax import lax
from jax.experimental import pallas as pl
from jax.experimental.pallas import tpu as pltpu
from jax.sharding import PartitionSpec as P

MESH = pl.DeviceIdType.MESH


def normalize(values, gain):
    return (
        values
        * lax.rsqrt(jnp.mean(values * values, axis=-1, keepdims=True) + 1e-06)
        * gain.astype(jnp.float32)
    )


def kernel(
    n, experts, chunks,
    normed, tokens, pick_map, out_map, weight_hi, weight_lo, gain, gate_hbm, up_hbm, down_hbm,
    moe_out, encoded_all,
    gate_w, up_w, down_w, normed_all, gathered, hidden, part, sums, summed, outbound, returned, encoded,
    load_sem, ag_send, ag_recv, z_send, z_recv, rs_send, rs_recv, back_send, back_recv, enc_send, enc_recv,
):
    p = lax.axis_index("dp")
    me = lax.axis_index("expert")
    rows, width = normed.shape
    cap = pick_map.shape[0]
    slots = outbound.shape[1]
    ff = gate_w.shape[1]
    chips = experts // 2
    core = lax.rem(me, 2)
    chip = lax.div(me, 2)
    partner = chip * 2 + (1 - core)
    ch_rows = cap // chunks

    loads = [
        pltpu.make_async_copy(src.at[0], dst, load_sem.at[i])
        for i, (src, dst) in enumerate(((gate_hbm, gate_w), (up_hbm, up_w), (down_hbm, down_w)))
    ]
    for load in loads:
        load.start()

    barrier = pltpu.get_barrier_semaphore()

    @pl.loop(1, experts)
    def _(k):
        pl.semaphore_signal(barrier, inc=1, device_id={"expert": lax.rem(me + k, experts)}, device_id_type=MESH)

    @pl.when(p > 0)
    def _():
        pl.semaphore_signal(barrier, inc=1, device_id={"dp": p - 1}, device_id_type=MESH)

    @pl.when(p < n - 1)
    def _():
        pl.semaphore_signal(barrier, inc=1, device_id={"dp": p + 1}, device_id_type=MESH)

    neighbours = jnp.where(p > 0, 1, 0) + jnp.where(p < n - 1, 1, 0)
    pl.semaphore_wait(barrier, experts - 1 + neighbours)

    def span(index, size):
        return pl.ds(pl.multiple_of(index * size, size), size)

    def plane_gather(own, full, send, recv):
        def copy(source, src, target, slot):
            return pltpu.make_async_remote_copy(
                src_ref=src,
                dst_ref=full.at[span(source, rows)],
                send_sem=send.at[slot],
                recv_sem=recv.at[source],
                device_id={"expert": target},
                device_id_type=MESH,
            )

        @pl.loop(1, chips)
        def _(k):
            copy(me, own, lax.rem(chip + k, chips) * 2 + core, k).start()

        copy(me, own, partner, 0).start()
        full[span(me, rows)] = own[...]

        @pl.loop(1, chips)
        def _(k):
            source = lax.rem(chip + chips - k, chips) * 2 + core
            piece = copy(source, full.at[span(source, rows)], partner, chips + k)
            piece.wait_recv()
            piece.start()

        copy(partner, own, partner, 0).wait_recv()

        @pl.loop(1, chips)
        def _(k):
            copy(lax.rem(chip + chips - k, chips) * 2 + 1 - core, own, partner, 0).wait_recv()

        copy(me, own, partner, 0).wait_send()

        @pl.loop(1, chips)
        def _(k):
            copy(me, own, partner, k).wait_send()
            copy(me, own, partner, chips + k).wait_send()

    with jax.named_scope("gather_normed"):
        plane_gather(normed, normed_all, ag_send, ag_recv)

    tile = 512

    @pl.loop(0, width // tile)
    def _(i):
        cols = span(i, tile)
        gathered[p, :, cols] = jnp.dot(
            pick_map[...], normed_all[:, cols], preferred_element_type=jnp.float32
        ).astype(jnp.bfloat16)

    def z_copy(g, c, way, target):
        piece = gathered.at[g, span(c, ch_rows)]
        return pltpu.make_async_remote_copy(
            src_ref=piece,
            dst_ref=piece,
            send_sem=z_send.at[way, g, c],
            recv_sem=z_recv.at[g, c],
            device_id={"dp": target},
            device_id_type=MESH,
        )

    def rs_copy(g, c, slot, target):
        return pltpu.make_async_remote_copy(
            src_ref=part.at[g, span(c, ch_rows)],
            dst_ref=sums.at[slot, span(c, ch_rows)],
            send_sem=rs_send.at[g, c],
            recv_sem=rs_recv.at[slot, c],
            device_id={"dp": target},
            device_id_type=MESH,
        )

    def rs_start(g, c):
        @pl.when(g < p)
        def _():
            rs_copy(g, c, g, p - 1).start()

        @pl.when(g > p)
        def _():
            rs_copy(g, c, jnp.where(g == p + 1, n, g), p + 1).start()

    @pl.loop(0, chunks)
    def _(c):
        @pl.when(p < n - 1)
        def _():
            z_copy(p, c, 0, p + 1).start()

        @pl.when(p > 0)
        def _():
            z_copy(p, c, 1, p - 1).start()

    for load in loads:
        load.wait()

    ff_tile = 256 if ff % 256 == 0 else 128

    @pl.loop(0, 2 * n - 1)
    def _(j):
        k = lax.div(j + 1, 2)
        odd = lax.rem(j, 2)
        g = p + k * (1 - 2 * odd)

        @pl.when((g >= 0) & (g < n))
        def _():
            @pl.loop(0, chunks)
            def _(c):
                @pl.when(g != p)
                def _():
                    z_copy(g, c, 0, p).wait_recv()

                @pl.when((g < p) & (p < n - 1))
                def _():
                    z_copy(g, c, 0, p + 1).start()

                @pl.when((g > p) & (p > 0))
                def _():
                    z_copy(g, c, 1, p - 1).start()

            @pl.loop(0, ff // ff_tile)
            def _(i):
                cols = span(i, ff_tile)
                block = gathered[g]
                gate = jnp.dot(block, gate_w[:, cols], preferred_element_type=jnp.float32)
                up = jnp.dot(block, up_w[:, cols], preferred_element_type=jnp.float32)
                hidden[:, cols] = (jax.nn.gelu(gate, approximate=True) * up).astype(jnp.bfloat16)

            @pl.loop(0, width // tile)
            def _(i):
                cols = span(i, tile)
                part[g, :, cols] = jnp.dot(
                    hidden[...], down_w[:, cols], preferred_element_type=jnp.float32
                ).astype(jnp.bfloat16)

            @pl.when(((g < p) & (p == n - 1)) | ((g > p) & (p == 0)))
            def _():
                @pl.loop(0, chunks)
                def _(c):
                    rs_start(g, c)

    left_first = jnp.where(2 * p >= n - 1, 1, 0)

    @pl.loop(0, 2 * (n - 1))
    def _(j):
        is_left = jnp.where(j < n - 1, left_first, 1 - left_first)
        g = p + (1 + lax.rem(j, n - 1)) * (1 - 2 * is_left)
        inner = jnp.where(is_left == 1, (g >= 0) & (p < n - 1), (g < n) & (p > 0))

        @pl.when(inner)
        def _():
            @pl.loop(0, chunks)
            def _(c):
                piece = span(c, ch_rows)
                rs_copy(g, c, g, p).wait_recv()
                part[g, piece] = (
                    part[g, piece].astype(jnp.float32) + sums[g, piece].astype(jnp.float32)
                ).astype(jnp.bfloat16)
                rs_start(g, c)

    @pl.loop(0, chunks)
    def _(c):
        piece = span(c, ch_rows)

        @pl.when(p < n - 1)
        def _():
            rs_copy(p, c, p, p).wait_recv()

        @pl.when(p > 0)
        def _():
            rs_copy(p, c, n, p).wait_recv()

        @pl.when((p > 0) & (p < n - 1))
        def _():
            summed[piece] = (
                part[p, piece].astype(jnp.float32)
                + sums[p, piece].astype(jnp.float32)
                + sums[n, piece].astype(jnp.float32)
            ).astype(jnp.bfloat16)

        @pl.when((p > 0) & (p == n - 1))
        def _():
            summed[piece] = (
                part[p, piece].astype(jnp.float32) + sums[n, piece].astype(jnp.float32)
            ).astype(jnp.bfloat16)

        @pl.when((p == 0) & (p < n - 1))
        def _():
            summed[piece] = (
                part[p, piece].astype(jnp.float32) + sums[p, piece].astype(jnp.float32)
            ).astype(jnp.bfloat16)

    def back_copy(source, target):
        return pltpu.make_async_remote_copy(
            src_ref=outbound.at[target],
            dst_ref=returned.at[span(source, slots)],
            send_sem=back_send.at[target],
            recv_sem=back_recv.at[source],
            device_id={"expert": target},
            device_id_type=MESH,
        )

    @pl.loop(1, experts + 1)
    def _(k):
        target = lax.rem(me + k, experts)
        outbound[target] = jnp.dot(
            out_map[span(target, slots)], summed[...], preferred_element_type=jnp.float32
        ).astype(jnp.bfloat16)

        @pl.when(k < experts)
        def _():
            back_copy(me, target).start()

    returned[span(me, slots)] = outbound[me]

    @pl.loop(1, experts)
    def _(k):
        back_copy(lax.rem(me + k, experts), me).wait_recv()

    square = jnp.zeros((rows, 1), jnp.float32)
    for i in range(width // tile):
        cols = pl.ds(i * tile, tile)
        block = returned[:, cols]
        value = (
            tokens[:, cols].astype(jnp.float32)
            + jnp.dot(weight_hi[...], block, preferred_element_type=jnp.float32)
            + jnp.dot(weight_lo[...], block, preferred_element_type=jnp.float32)
        ).astype(jnp.bfloat16)
        moe_out[:, cols] = value
        wide = value.astype(jnp.float32)
        square = square + jnp.sum(wide * wide, axis=1, keepdims=True)
    scale = lax.rsqrt(square / width + 1e-06)
    for i in range(width // tile):
        cols = pl.ds(i * tile, tile)
        encoded[:, cols] = (
            moe_out[:, cols].astype(jnp.float32) * scale * gain[:, cols].astype(jnp.float32)
        ).astype(jnp.bfloat16)

    with jax.named_scope("gather_encoded"):
        plane_gather(encoded, encoded_all, enc_send, enc_recv)

    @pl.loop(1, experts)
    def _(k):
        back_copy(me, lax.rem(me + k, experts)).wait_send()

    @pl.loop(0, n)
    def _(g):
        @pl.loop(0, chunks)
        def _(c):
            @pl.when((g <= p) & (p < n - 1))
            def _():
                z_copy(g, c, 0, p).wait_send()

            @pl.when((g >= p) & (p > 0))
            def _():
                z_copy(g, c, 1, p).wait_send()

            @pl.when(g != p)
            def _():
                rs_copy(g, c, g, p).wait_send()


def local(
    tokens,
    norm_gain,
    router_weight,
    gate_weight,
    up_weight,
    down_weight,
    expert_picks,
    final_gain,
    kv_weight,
):
    n = lax.axis_size("dp")
    experts = lax.axis_size("expert")
    me = lax.axis_index("expert")
    rows, width = tokens.shape
    ff = gate_weight.shape[2]
    chosen = expert_picks[0]
    cap = chosen.shape[1]
    slots = 4 * rows // experts
    wide_tokens = tokens.astype(jnp.float32)
    normed = normalize(wide_tokens, norm_gain).astype(jnp.bfloat16)
    gate_probs = jax.nn.sigmoid(jnp.dot(normed, router_weight, preferred_element_type=jnp.float32))
    source = chosen // rows
    local_row = chosen % rows
    positions = jnp.arange(cap, dtype=jnp.int32)
    earlier = (source[:, :, None] == source[:, None, :]) & (
        positions[None, None, :] < positions[None, :, None]
    )
    slot_rank = jnp.sum(earlier.astype(jnp.int32), axis=2)
    own_chosen = lax.dynamic_index_in_dim(chosen, me, 0, keepdims=False)
    own_rank = lax.dynamic_index_in_dim(slot_rank, me, 0, keepdims=False)
    own_slot = (own_chosen // rows) * slots + own_rank
    pick_map = (own_chosen[:, None] == jnp.arange(experts * rows, dtype=jnp.int32)[None, :]).astype(jnp.bfloat16)
    out_map = (jnp.arange(experts * slots, dtype=jnp.int32)[:, None] == own_slot[None, :]).astype(jnp.bfloat16)
    send_slot = (
        (source == me)[:, :, None] & (slot_rank[:, :, None] == jnp.arange(slots, dtype=jnp.int32))
    ).astype(jnp.bfloat16)
    local_map = (local_row[:, :, None] == jnp.arange(rows, dtype=jnp.int32)).astype(jnp.bfloat16)
    send_map = jnp.einsum("ecm,ect->tem", send_slot, local_map, preferred_element_type=jnp.float32)
    weight = (send_map * gate_probs[:, :, None]).reshape(rows, experts * slots)
    weight_hi = lax.reduce_precision(weight, 8, 7)
    weight_lo = (weight - weight_hi).astype(jnp.bfloat16)
    weight_hi = weight_hi.astype(jnp.bfloat16)

    chunks = 4
    bf16 = jnp.bfloat16
    dma = pltpu.SemaphoreType.DMA
    vmem = pl.BlockSpec(memory_space=pltpu.VMEM)
    hbm = pl.BlockSpec(memory_space=pl.ANY)
    moe_out, encoded_all = pl.pallas_call(
        functools.partial(kernel, n, experts, chunks),
        out_shape=(
            jax.ShapeDtypeStruct((rows, width), bf16),
            jax.ShapeDtypeStruct((experts * rows, width), bf16),
        ),
        in_specs=[vmem] * 7 + [hbm] * 3,
        out_specs=(vmem, vmem),
        scratch_shapes=[
            pltpu.VMEM((width, ff), bf16),
            pltpu.VMEM((width, ff), bf16),
            pltpu.VMEM((ff, width), bf16),
            pltpu.VMEM((experts * rows, width), bf16),
            pltpu.VMEM((n, cap, width), bf16),
            pltpu.VMEM((cap, ff), bf16),
            pltpu.VMEM((n, cap, width), bf16),
            pltpu.VMEM((n + 1, cap, width), bf16),
            pltpu.VMEM((cap, width), bf16),
            pltpu.VMEM((experts, slots, width), bf16),
            pltpu.VMEM((experts * slots, width), bf16),
            pltpu.VMEM((rows, width), bf16),
            dma((3,)),
            dma((experts,)),
            dma((experts,)),
            dma((2, n, chunks)),
            dma((n, chunks)),
            dma((n, chunks)),
            dma((n + 1, chunks)),
            dma((experts,)),
            dma((experts,)),
            dma((experts,)),
            dma((experts,)),
        ],
        compiler_params=pltpu.CompilerParams(
            collective_id=0, has_side_effects=True, vmem_limit_bytes=60 * 1024 * 1024
        ),
    )(
        normed, tokens, pick_map, out_map, weight_hi, weight_lo, final_gain[None, :],
        gate_weight, up_weight, down_weight,
    )
    kv_matrix = kv_weight.reshape(kv_weight.shape[0], -1)
    kv_rows = lax.dot_general(
        kv_matrix, encoded_all, (((0,), (1,)), ((), ())), preferred_element_type=jnp.float32
    ).astype(jnp.bfloat16)
    kv_cache = kv_rows.T.reshape((encoded_all.shape[0],) + kv_weight.shape[1:])
    return (moe_out, kv_cache)


def solution(mesh):
    in_specs = (
        P(("dp", "expert"), None),
        P(),
        P(),
        P("expert", None, "dp"),
        P("expert", None, "dp"),
        P("expert", "dp", None),
        P("dp", None, None),
        P(),
        P(None, "expert", None, None, None),
    )
    out_specs = (P(("dp", "expert"), None), P("dp", "expert", None, None, None))
    return jax.shard_map(local, mesh=mesh, in_specs=in_specs, out_specs=out_specs, check_vma=False)
```

```python
import functools

import jax
import jax.numpy as jnp
from jax import lax
from jax.experimental import pallas as pl
from jax.experimental.pallas import tpu as pltpu
from jax.sharding import PartitionSpec as P

MESH = pl.DeviceIdType.MESH


def normalize(values, gain):
    return (
        values
        * lax.rsqrt(jnp.mean(values * values, axis=-1, keepdims=True) + 1e-06)
        * gain.astype(jnp.float32)
    )


def kernel(
    n, experts, chunks,
    normed, tokens, pick_map, out_map, weight_hi, weight_lo, gate_hbm, up_hbm, down_hbm,
    moe_out, encoded_all,
    gate_w, up_w, down_w, normed_all, gathered, hidden, part, sums, outbound, returned, encoded,
    load_sem, ag_send, ag_recv, z_send, z_recv, rs_send, rs_recv, back_send, back_recv, enc_send, enc_recv,
):
    p = lax.axis_index("dp")
    me = lax.axis_index("expert")
    rows, width = normed.shape
    cap = pick_map.shape[0]
    slots = outbound.shape[0] // experts
    ff = gate_w.shape[1]
    chips = experts // 2
    core = lax.rem(me, 2)
    chip = lax.div(me, 2)
    partner = chip * 2 + (1 - core)

    loads = [
        pltpu.make_async_copy(src.at[0], dst, load_sem.at[i])
        for i, (src, dst) in enumerate(((gate_hbm, gate_w), (up_hbm, up_w), (down_hbm, down_w)))
    ]
    for load in loads:
        load.start()

    barrier = pltpu.get_barrier_semaphore()

    @pl.loop(1, experts)
    def _(k):
        pl.semaphore_signal(barrier, inc=1, device_id={"expert": lax.rem(me + k, experts)}, device_id_type=MESH)

    @pl.when(p > 0)
    def _():
        pl.semaphore_signal(barrier, inc=1, device_id={"dp": p - 1}, device_id_type=MESH)

    @pl.when(p < n - 1)
    def _():
        pl.semaphore_signal(barrier, inc=1, device_id={"dp": p + 1}, device_id_type=MESH)

    neighbours = jnp.where(p > 0, 1, 0) + jnp.where(p < n - 1, 1, 0)
    pl.semaphore_wait(barrier, experts - 1 + neighbours)

    def span(index, size):
        return pl.ds(pl.multiple_of(index * size, size), size)

    tile = width // chunks

    def plane_copy(own, full, send, recv, c, source, target, slot, relay=False):
        cols = span(c, tile)
        place = full.at[span(source, rows), cols]
        return pltpu.make_async_remote_copy(
            src_ref=place if relay else own.at[:, cols],
            dst_ref=place,
            send_sem=send.at[slot, c],
            recv_sem=recv.at[source, c],
            device_id={"expert": target},
            device_id_type=MESH,
        )

    def plane_start(args, c):
        @pl.loop(1, chips)
        def _(k):
            plane_copy(*args, c, me, lax.rem(chip + k, chips) * 2 + core, k).start()

        plane_copy(*args, c, me, partner, 0).start()

    def plane_relay(args, c):
        @pl.loop(1, chips)
        def _(k):
            source = lax.rem(chip + chips - k, chips) * 2 + core
            piece = plane_copy(*args, c, source, partner, chips + k, relay=True)
            piece.wait_recv()
            piece.start()

    def plane_arrive(args, c):
        @pl.loop(0, chips)
        def _(k):
            plane_copy(*args, c, lax.rem(chip + k, chips) * 2 + 1 - core, partner, 0).wait_recv()

    def plane_finish(args, c):
        @pl.loop(0, chips)
        def _(k):
            plane_copy(*args, c, me, partner, k).wait_send()

        @pl.loop(1, chips)
        def _(k):
            plane_copy(*args, c, me, partner, chips + k).wait_send()

    first = (normed, normed_all, ag_send, ag_recv)

    @pl.loop(0, chunks)
    def _(c):
        plane_start(first, c)

    normed_all[span(me, rows)] = normed[...]

    def z_copy(g, c, way, target):
        piece = gathered.at[g, :, span(c, tile)]
        return pltpu.make_async_remote_copy(
            src_ref=piece,
            dst_ref=piece,
            send_sem=z_send.at[way, g, c],
            recv_sem=z_recv.at[g, c],
            device_id={"dp": target},
            device_id_type=MESH,
        )

    def rs_copy(g, c, slot, target):
        return pltpu.make_async_remote_copy(
            src_ref=part.at[g, :, span(c, tile)],
            dst_ref=sums.at[slot, :, span(c, tile)],
            send_sem=rs_send.at[g, c],
            recv_sem=rs_recv.at[slot, c],
            device_id={"dp": target},
            device_id_type=MESH,
        )

    def rs_start(g, c):
        @pl.when(g < p)
        def _():
            rs_copy(g, c, g, p - 1).start()

        @pl.when(g > p)
        def _():
            rs_copy(g, c, jnp.where(g == p + 1, n, g), p + 1).start()

    @pl.loop(0, chunks)
    def _(c):
        plane_relay(first, c)
        plane_arrive(first, c)
        gathered[p, :, span(c, tile)] = jnp.dot(
            pick_map[...], normed_all[:, span(c, tile)], preferred_element_type=jnp.float32
        ).astype(jnp.bfloat16)

        @pl.when(p < n - 1)
        def _():
            z_copy(p, c, 0, p + 1).start()

        @pl.when(p > 0)
        def _():
            z_copy(p, c, 1, p - 1).start()

    for load in loads:
        load.wait()

    ff_tile = 256 if ff % 256 == 0 else 128

    @pl.loop(0, 2 * n - 1)
    def _(j):
        k = lax.div(j + 1, 2)
        odd = lax.rem(j, 2)
        g = p + k * (1 - 2 * odd)

        @pl.when((g >= 0) & (g < n))
        def _():
            @pl.loop(0, chunks)
            def _(c):
                @pl.when(g != p)
                def _():
                    z_copy(g, c, 0, p).wait_recv()

                @pl.when((g < p) & (p < n - 1))
                def _():
                    z_copy(g, c, 0, p + 1).start()

                @pl.when((g > p) & (p > 0))
                def _():
                    z_copy(g, c, 1, p - 1).start()

            @pl.loop(0, ff // ff_tile)
            def _(i):
                cols = span(i, ff_tile)
                block = gathered[g]
                gate = jnp.dot(block, gate_w[:, cols], preferred_element_type=jnp.float32)
                up = jnp.dot(block, up_w[:, cols], preferred_element_type=jnp.float32)
                hidden[:, cols] = (jax.nn.gelu(gate, approximate=True) * up).astype(jnp.bfloat16)

            @pl.loop(0, chunks)
            def _(c):
                cols = span(c, tile)
                part[g, :, cols] = jnp.dot(
                    hidden[...], down_w[:, cols], preferred_element_type=jnp.float32
                ).astype(jnp.bfloat16)

                @pl.when(((g < p) & (p == n - 1)) | ((g > p) & (p == 0)))
                def _():
                    rs_start(g, c)

    left_first = jnp.where(2 * p >= n - 1, 1, 0)

    @pl.loop(0, 2 * (n - 1))
    def _(j):
        is_left = jnp.where(j < n - 1, left_first, 1 - left_first)
        g = p + (1 + lax.rem(j, n - 1)) * (1 - 2 * is_left)
        inner = jnp.where(is_left == 1, (g >= 0) & (p < n - 1), (g < n) & (p > 0))

        @pl.when(inner)
        def _():
            @pl.loop(0, chunks)
            def _(c):
                piece = span(c, tile)
                rs_copy(g, c, g, p).wait_recv()
                part[g, :, piece] = (
                    part[g, :, piece].astype(jnp.float32) + sums[g, :, piece].astype(jnp.float32)
                ).astype(jnp.bfloat16)
                rs_start(g, c)

    def back_copy(c, source, target):
        cols = span(c, tile)
        return pltpu.make_async_remote_copy(
            src_ref=outbound.at[span(target, slots), cols],
            dst_ref=returned.at[span(source, slots), cols],
            send_sem=back_send.at[target, c],
            recv_sem=back_recv.at[source, c],
            device_id={"expert": target},
            device_id_type=MESH,
        )

    second = (encoded, encoded_all, enc_send, enc_recv)

    @pl.loop(0, chunks + 2)
    def _(step):
        @pl.when(step < chunks)
        def _():
            c = step
            cols = span(c, tile)

            @pl.when(p < n - 1)
            def _():
                rs_copy(p, c, p, p).wait_recv()
                part[p, :, cols] = (
                    part[p, :, cols].astype(jnp.float32) + sums[p, :, cols].astype(jnp.float32)
                ).astype(jnp.bfloat16)

            @pl.when(p > 0)
            def _():
                rs_copy(p, c, n, p).wait_recv()
                part[p, :, cols] = (
                    part[p, :, cols].astype(jnp.float32) + sums[n, :, cols].astype(jnp.float32)
                ).astype(jnp.bfloat16)

            outbound[:, cols] = jnp.dot(
                out_map[...], part[p, :, cols], preferred_element_type=jnp.float32
            ).astype(jnp.bfloat16)

            @pl.loop(1, experts)
            def _(k):
                back_copy(c, me, lax.rem(me + k, experts)).start()

            returned[span(me, slots), cols] = outbound[span(me, slots), cols]

        @pl.when((step > 0) & (step <= chunks))
        def _():
            c = step - 1
            cols = span(c, tile)

            @pl.loop(1, experts)
            def _(k):
                back_copy(c, lax.rem(me + k, experts), me).wait_recv()

            block = returned[:, cols]
            value = (
                tokens[:, cols].astype(jnp.float32)
                + jnp.dot(weight_hi[...], block, preferred_element_type=jnp.float32)
                + jnp.dot(weight_lo[...], block, preferred_element_type=jnp.float32)
            ).astype(jnp.bfloat16)
            moe_out[:, cols] = value
            encoded[:, cols] = value
            encoded_all[span(me, rows), cols] = value
            plane_start(second, c)

        @pl.when(step > 1)
        def _():
            plane_relay(second, step - 2)

    @pl.loop(0, chunks)
    def _(c):
        plane_arrive(second, c)

    @pl.loop(0, chunks)
    def _(c):
        plane_finish(first, c)
        plane_finish(second, c)

        @pl.loop(1, experts)
        def _(k):
            back_copy(c, me, lax.rem(me + k, experts)).wait_send()

    @pl.loop(0, n)
    def _(g):
        @pl.loop(0, chunks)
        def _(c):
            @pl.when((g <= p) & (p < n - 1))
            def _():
                z_copy(g, c, 0, p).wait_send()

            @pl.when((g >= p) & (p > 0))
            def _():
                z_copy(g, c, 1, p).wait_send()

            @pl.when(g != p)
            def _():
                rs_copy(g, c, g, p).wait_send()


def kv_kernel(moe_all, gain, weight, out, encoded):
    rows, width = moe_all.shape
    step = 128

    @pl.loop(0, rows // step)
    def _(i):
        piece = pl.ds(pl.multiple_of(i * step, step), step)
        encoded[piece] = normalize(moe_all[piece].astype(jnp.float32), gain[...]).astype(jnp.bfloat16)

    @pl.loop(0, weight.shape[0] // step)
    def _(i):
        piece = pl.ds(pl.multiple_of(i * step, step), step)
        out[piece] = lax.dot_general(
            weight[piece], encoded[...], (((1,), (1,)), ((), ())), preferred_element_type=jnp.float32
        ).astype(jnp.bfloat16)


def local(
    tokens,
    norm_gain,
    router_weight,
    gate_weight,
    up_weight,
    down_weight,
    expert_picks,
    final_gain,
    kv_weight,
):
    n = lax.axis_size("dp")
    experts = lax.axis_size("expert")
    me = lax.axis_index("expert")
    rows, width = tokens.shape
    ff = gate_weight.shape[2]
    chosen = expert_picks[0]
    cap = chosen.shape[1]
    slots = 4 * rows // experts
    wide_tokens = tokens.astype(jnp.float32)
    normed = normalize(wide_tokens, norm_gain).astype(jnp.bfloat16)
    gate_probs = jax.nn.sigmoid(jnp.dot(normed, router_weight, preferred_element_type=jnp.float32))
    source = chosen // rows
    local_row = chosen % rows
    positions = jnp.arange(cap, dtype=jnp.int32)
    earlier = (source[:, :, None] == source[:, None, :]) & (
        positions[None, None, :] < positions[None, :, None]
    )
    slot_rank = jnp.sum(earlier.astype(jnp.int32), axis=2)
    own_chosen = lax.dynamic_index_in_dim(chosen, me, 0, keepdims=False)
    own_rank = lax.dynamic_index_in_dim(slot_rank, me, 0, keepdims=False)
    own_slot = (own_chosen // rows) * slots + own_rank
    pick_map = (own_chosen[:, None] == jnp.arange(experts * rows, dtype=jnp.int32)[None, :]).astype(jnp.bfloat16)
    out_map = (jnp.arange(experts * slots, dtype=jnp.int32)[:, None] == own_slot[None, :]).astype(jnp.bfloat16)
    send_slot = (
        (source == me)[:, :, None] & (slot_rank[:, :, None] == jnp.arange(slots, dtype=jnp.int32))
    ).astype(jnp.bfloat16)
    local_map = (local_row[:, :, None] == jnp.arange(rows, dtype=jnp.int32)).astype(jnp.bfloat16)
    send_map = jnp.einsum("ecm,ect->tem", send_slot, local_map, preferred_element_type=jnp.float32)
    weight = (send_map * gate_probs[:, :, None]).reshape(rows, experts * slots)
    weight_hi = lax.reduce_precision(weight, 8, 7)
    weight_lo = (weight - weight_hi).astype(jnp.bfloat16)
    weight_hi = weight_hi.astype(jnp.bfloat16)

    chunks = 4
    bf16 = jnp.bfloat16
    dma = pltpu.SemaphoreType.DMA
    vmem = pl.BlockSpec(memory_space=pltpu.VMEM)
    hbm = pl.BlockSpec(memory_space=pl.ANY)
    moe_out, moe_all = pl.pallas_call(
        functools.partial(kernel, n, experts, chunks),
        out_shape=(
            jax.ShapeDtypeStruct((rows, width), bf16),
            jax.ShapeDtypeStruct((experts * rows, width), bf16),
        ),
        in_specs=[vmem] * 6 + [hbm] * 3,
        out_specs=(vmem, vmem),
        scratch_shapes=[
            pltpu.VMEM((width, ff), bf16),
            pltpu.VMEM((width, ff), bf16),
            pltpu.VMEM((ff, width), bf16),
            pltpu.VMEM((experts * rows, width), bf16),
            pltpu.VMEM((n, cap, width), bf16),
            pltpu.VMEM((cap, ff), bf16),
            pltpu.VMEM((n, cap, width), bf16),
            pltpu.VMEM((n + 1, cap, width), bf16),
            pltpu.VMEM((experts * slots, width), bf16),
            pltpu.VMEM((experts * slots, width), bf16),
            pltpu.VMEM((rows, width), bf16),
            dma((3,)),
            dma((experts, chunks)),
            dma((experts, chunks)),
            dma((2, n, chunks)),
            dma((n, chunks)),
            dma((n, chunks)),
            dma((n + 1, chunks)),
            dma((experts, chunks)),
            dma((experts, chunks)),
            dma((experts, chunks)),
            dma((experts, chunks)),
        ],
        compiler_params=pltpu.CompilerParams(
            collective_id=0, has_side_effects=True, vmem_limit_bytes=60 * 1024 * 1024
        ),
    )(
        normed, tokens, pick_map, out_map, weight_hi, weight_lo,
        gate_weight, up_weight, down_weight,
    )
    all_rows = moe_all.shape[0]
    kv_matrix = kv_weight.reshape(width, -1).T
    kv_rows = pl.pallas_call(
        kv_kernel,
        out_shape=jax.ShapeDtypeStruct((kv_matrix.shape[0], all_rows), bf16),
        in_specs=[vmem] * 3,
        out_specs=vmem,
        scratch_shapes=[pltpu.VMEM((all_rows, width), bf16)],
        compiler_params=pltpu.CompilerParams(vmem_limit_bytes=40 * 1024 * 1024),
    )(moe_all, final_gain[None, :], kv_matrix)
    kv_cache = kv_rows.T.reshape((all_rows,) + kv_weight.shape[1:])
    return (moe_out, kv_cache)


def solution(mesh):
    in_specs = (
        P(("dp", "expert"), None),
        P(),
        P(),
        P("expert", None, "dp"),
        P("expert", None, "dp"),
        P("expert", "dp", None),
        P("dp", None, None),
        P(),
        P(None, "expert", None, None, None),
    )
    out_specs = (P(("dp", "expert"), None), P("dp", "expert", None, None, None))
    return jax.shard_map(local, mesh=mesh, in_specs=in_specs, out_specs=out_specs, check_vma=False)
```
